32 devices in a mesh: dp: 4 (over z), ctx: 8 (over y, x, core).
Axes of the slice: x: 2, y: 2, z: 4, core: 2. Of those that a mesh axis runs over, the one named last changes fastest.
Arguments:
- tokens: bfloat16 [4, 4096, 1024], P('dp', 'ctx'), may hold values from -60 to 60
- kept: int32 [4, 2048], P('dp', 'ctx'), may hold values from 0 to 4095, as said below
- gain_attn: float32 [1024], replicated, may hold values from 0.25 to 1.75
- gain_ffn: float32 [1024], replicated, may hold values from 0.25 to 1.75
- w_query: bfloat16 [1024, 512], P(None, 'ctx'), may hold values from -4 to 4
- w_key: bfloat16 [1024, 512], P(None, 'ctx'), may hold values from -4 to 4
- w_value: bfloat16 [1024, 512], P(None, 'ctx'), may hold values from -0.1875 to 0.1875
- w_out: bfloat16 [512, 1024], P('ctx'), may hold values from -0.25 to 0.25
- expert_ids: int32 [4, 2048, 1], P('dp', 'ctx'), may hold values from 0 to 31; in each aligned block of 256 rows (0 to 255, 256 to 511, ..., all dimensions but the last counted through in order) at most 16 rows name the same one
- w_in: bfloat16 [32, 1024, 2816], P(('dp', 'ctx')), may hold values from -0.1875 to 0.1875
- w_back: bfloat16 [32, 2816, 1024], P(('dp', 'ctx')), may hold values from -0.109375 to 0.109375
Outputs:
- blended: bfloat16 [4, 4096, 1024], P('dp', 'ctx')
The draws below stay inside these ranges and needn't reach their ends.
Inputs may be any that keep to these rules, and one draw needn't show every extreme that they name: `kept`: in each document row, entries j * 256 to (j + 1) * 256 - 1 are strictly increasing positions from j * 512 to (j + 1) * 512 - 1. `expert_ids`: in each aligned block of 256 rows (the kept positions of one block b) no expert is named more than 16 times.
All inputs are finite; a program needn't handle non-finite values.
Results may differ from the reference program's by a relative error of at most 0.007.
Values may be sent and summed in bfloat16 or wider, within the bound.
A program may use at most 64 MiB of HBM per device.

```python
import math
import jax
import jax.numpy as jnp
import numpy as np
from jax import lax

D = 1024
HS = 64
FF = 2816
SHARD_DEV = 512
HEADS = 8
EXPERTS = 32
INNER = 512
KEEP_DEV = 256
KEEP = 2048
SEQ = 4096
DOCS = 4
CAP = 16
DEVICES = 32


def draw_tokens(key, part):
    noise = jax.random.normal(jax.random.fold_in(key, 1), (DOCS, SEQ, D), jnp.float32)
    return jnp.clip(noise, -6.0, 6.0).astype(jnp.bfloat16)


def draw_projection(key, salt):
    base = jax.random.normal(jax.random.fold_in(key, salt), (D, INNER), jnp.float32) / math.sqrt(D)
    return jnp.clip(base, -4.0, 4.0).astype(jnp.bfloat16)


def draw_w_query(key, part):
    return draw_projection(key, 3)


def draw_w_key(key, part):
    return draw_projection(key, 4)


def draw_kept(key, part):
    shards = SEQ // SHARD_DEV
    streams = jax.random.split(jax.random.fold_in(key, 5), DOCS * shards)

    def choose_some(stream):
        return jnp.sort(jax.random.permutation(stream, SHARD_DEV)[:KEEP_DEV].astype(jnp.int32))
    chosen = jax.vmap(choose_some)(streams).reshape(DOCS, shards, KEEP_DEV)
    offsets = (jnp.arange(shards, dtype=jnp.int32) * SHARD_DEV)[None, :, None]
    return (chosen + offsets).reshape(DOCS, KEEP).astype(jnp.int32)


def level_of(stream_key, shape, cuts, smallest, largest):
    level = 1.0
    for dim, parts in cuts:
        draws = jax.random.uniform(jax.random.fold_in(jax.random.fold_in(stream_key, 6), dim), (parts,), jnp.float32, smallest / len(cuts), largest / len(cuts))
        level = level * jnp.repeat(jnp.exp(draws), shape[dim] // parts).reshape((-1,) + (1,) * (len(shape) - 1 - dim))
    return level


def deal_out(own_key, own, number, rows, count, top, limit, skew):
    order = jax.random.permutation(own_key, count)
    crowded, ordinary = shares(count, rows * top, limit, skew, True), shares(count, rows * top, limit, skew, False)
    places = jnp.arange(count)

    def named(tallies, offset_by):
        used = int((tallies > 0).sum())
        fixed = max(1, used // 4)
        shifted = fixed + (places - fixed + offset_by * (used - fixed)) % max(1, count - fixed)
        return jnp.zeros((count,), jnp.int32).at[order[jnp.where(places < fixed, places, shifted)]].set(jnp.asarray(tallies, jnp.int32))

    tallies = jnp.where(number % 4 == 0, named(crowded, number // 4), named(ordinary, number - number // 4 - 1))
    mixed = jax.random.permutation(jax.random.fold_in(own, 3), count)
    donor, taker = mixed[0:count // 2 * 2:2], mixed[1:count // 2 * 2:2]
    room = jnp.minimum(tallies[donor] - 1, limit - tallies[taker]) // 2
    room = jnp.where((donor == order[0]) | (taker == order[0]) | (tallies[taker] == 0), 0, jnp.maximum(room, 0))
    shifted = jax.random.randint(jax.random.fold_in(own, 4), (count // 2,), 0, 1 << 20) % (room + 1)
    tallies = tallies.at[donor].add(-shifted).at[taker].add(shifted)
    labels = jnp.searchsorted(jnp.cumsum(tallies), jnp.arange(rows * top), side="right").astype(jnp.int32)
    table = labels.reshape(top, rows).T
    table = table[jax.random.permutation(jax.random.fold_in(own, 1), rows)]
    offset_by = jax.random.randint(jax.random.fold_in(own, 2), (rows, 1), 0, top)
    return jnp.take_along_axis(table, (jnp.arange(top)[None, :] + offset_by) % top, axis=1)


def shares(number_of, total, most, skew, full):
    portions = [(1 << 20) // math.isqrt(standing ** skew) + 1 for standing in range(1, number_of + 1)]
    largest = most if full else min(most, max(-(-total // number_of), total * portions[0] // sum(portions)))
    least = 1 if total - largest >= number_of - 1 else 0
    holding, rest = [largest] + [least] * (number_of - 1), total - largest - least * (number_of - 1)
    while rest > 0:
        movable = [i for i in range(1, number_of) if holding[i] < largest] or [i for i in range(1, number_of) if holding[i] < most]
        whole, budget = sum([portions[i] for i in movable]), rest
        for i in movable:
            addition = min(most - holding[i], max(1, budget * portions[i] // whole), rest)
            holding[i] = holding[i] + addition
            rest = rest - addition
    return np.array(holding)


def normal_values(stream_key, shape, deviation, limit, cuts=(), kind=jnp.bfloat16):
    level = level_of(stream_key, shape, cuts, -0.22, 0.18) if cuts else 1.0
    values = jax.random.normal(stream_key, shape, jnp.float32) * deviation * level
    return jnp.minimum(jnp.maximum(values, -limit), limit).astype(kind)


def setup_inputs(seed: int = 0) -> dict:
    splits = jax.random.split(jax.random.key(seed), 12)
    tokens = draw_tokens(jax.random.fold_in(splits[11], 71), 0)
    kept = draw_kept(jax.random.fold_in(splits[11], 71), 0)
    gain_attn = jnp.clip(1.0 + 0.15 * jax.random.normal(splits[2], (D,), jnp.float32), 0.25, 1.75)
    gain_ffn = jnp.clip(1.0 + 0.15 * jax.random.normal(splits[3], (D,), jnp.float32), 0.25, 1.75)
    w_query = draw_w_query(jax.random.fold_in(splits[11], 71), 0)
    w_key = draw_w_key(jax.random.fold_in(splits[11], 71), 0)
    w_value = normal_values(splits[6], (D, INNER), D ** -0.5, 0.1875, ((1, 8),))
    w_out = normal_values(splits[7], (INNER, D), INNER ** -0.5, 0.25, ((0, 8),))
    expert_ids_keys = jax.random.split(jax.random.fold_in(splits[8], 1), DOCS * KEEP // KEEP_DEV)
    expert_ids_turns = jax.random.permutation(jax.random.fold_in(splits[8], 3), DOCS * KEEP // KEEP_DEV)
    expert_ids = jax.vmap(lambda own, number: deal_out(jax.random.fold_in(splits[8], 2), own, number, KEEP_DEV, EXPERTS, 1, CAP, 1))(expert_ids_keys, expert_ids_turns).reshape((DOCS, KEEP, 1))
    w_in = normal_values(splits[9], (EXPERTS, D, FF), D ** -0.5, 0.1875, ((0, 32),))
    w_back = normal_values(splits[10], (EXPERTS, FF, D), FF ** -0.5, 0.109375, ((0, 32),))
    return {"tokens": tokens, "kept": kept, "gain_attn": gain_attn, "gain_ffn": gain_ffn, "w_query": w_query, "w_key": w_key, "w_value": w_value, "w_out": w_out, "expert_ids": expert_ids, "w_in": w_in, "w_back": w_back}


eps_norm = 1e-06
score_gain = 2.5

def rms_scale(values, gain):
    values = values.astype(jnp.float32)
    power = lax.optimization_barrier(jnp.mean(values * values, axis=-1, keepdims=True))
    return values * lax.rsqrt(power + eps_norm) * gain

def attend_document(triple):
    queries, keys, values = triple
    scale = score_gain / math.sqrt(HS)
    keys_wide = keys.astype(jnp.float32)
    values_wide = values.astype(jnp.float32)
    blocks = queries.reshape(KEEP // 512, 512, HEADS, HS)

    def one_block(block_rows):
        scores = jnp.einsum('qhd,khd->hqk', block_rows.astype(jnp.float32), keys_wide) * scale
        top = lax.optimization_barrier(jnp.max(scores, axis=-1, keepdims=True))
        weights = jnp.exp(scores - top)
        probs = (weights / lax.optimization_barrier(jnp.sum(weights, axis=-1, keepdims=True))).astype(jnp.bfloat16)
        mixed = jnp.einsum('hqk,khd->qhd', probs.astype(jnp.float32), values_wide)
        return mixed.astype(jnp.bfloat16)
    return lax.map(one_block, blocks).reshape(KEEP, HEADS * HS)

def reference(tokens, kept, gain_attn, gain_ffn, w_query, w_key, w_value, w_out, expert_ids, w_in, w_back):
    rows = jax.vmap(lambda doc, where: jnp.take(doc, where, axis=0))(tokens, kept)
    normed = rms_scale(rows, gain_attn).astype(jnp.bfloat16).reshape(DOCS * KEEP, D)
    queries = jnp.dot(normed, w_query, preferred_element_type=jnp.float32).astype(jnp.bfloat16)
    keys = jnp.dot(normed, w_key, preferred_element_type=jnp.float32).astype(jnp.bfloat16)
    values = jnp.dot(normed, w_value, preferred_element_type=jnp.float32).astype(jnp.bfloat16)
    shape4 = (DOCS, KEEP, HEADS, HS)
    mixed = lax.map(attend_document, (queries.reshape(shape4), keys.reshape(shape4), values.reshape(shape4)))
    attn = jnp.dot(mixed.reshape(DOCS * KEEP, INNER), w_out, preferred_element_type=jnp.float32)
    first = rows.reshape(DOCS * KEEP, D).astype(jnp.float32) + attn
    ffn_in = rms_scale(first, gain_ffn).astype(jnp.bfloat16)
    ids = expert_ids.reshape(DEVICES, KEEP_DEV).astype(jnp.int32)
    onehot = (ids[:, :, None] == jnp.arange(EXPERTS, dtype=jnp.int32)[None, None, :]).astype(jnp.int32)
    before = jnp.cumsum(onehot, axis=1) - onehot
    slots = lax.optimization_barrier(jnp.sum(before * onehot, axis=2)).astype(jnp.int32)
    place = (ids * CAP + slots).astype(jnp.int32)
    source = jnp.broadcast_to(jnp.arange(DEVICES, dtype=jnp.int32)[:, None], (DEVICES, KEEP_DEV))
    buffers = jnp.zeros((DEVICES, EXPERTS * CAP, D), jnp.bfloat16)
    buffers = buffers.at[source, place].set(ffn_in.reshape(DEVICES, KEEP_DEV, D))
    slabs = jnp.transpose(buffers.reshape(DEVICES, EXPERTS, CAP, D), (1, 0, 2, 3))

    def run_expert(args):
        slab, first_weight, second_weight = args
        flat_in = slab.reshape(DEVICES * CAP, D)
        hidden = jnp.maximum(jnp.dot(flat_in, first_weight, preferred_element_type=jnp.float32), 0.0)
        hidden = hidden.astype(jnp.bfloat16)
        answer = jnp.dot(hidden, second_weight, preferred_element_type=jnp.float32).astype(jnp.bfloat16)
        return answer.reshape(DEVICES, CAP, D)
    answers = lax.map(run_expert, (slabs, w_in, w_back))
    back = jnp.transpose(answers, (1, 0, 2, 3)).reshape(DEVICES, EXPERTS * CAP, D)
    taken = jnp.take_along_axis(back, place[:, :, None], axis=1)
    second = (first + taken.reshape(DOCS * KEEP, D).astype(jnp.float32)).astype(jnp.bfloat16)
    second = second.reshape(DOCS, KEEP, D)
    return jax.vmap(lambda doc, where, fresh: doc.at[where].set(fresh))(tokens, kept, second)
```

```python
import functools
import math

import jax
import jax.numpy as jnp
from jax import lax
from jax.experimental import pallas as pl
from jax.experimental.pallas import tpu as pltpu
from jax.sharding import PartitionSpec as P

HS = 64
MESH = pl.DeviceIdType.MESH

eps_norm = 1e-06
score_gain = 2.5


def rms_scale(values, gain):
    values = values.astype(jnp.float32)
    power = jnp.mean(values * values, axis=-1, keepdims=True)
    return values * lax.rsqrt(power + eps_norm) * gain


class Gather:
    def __init__(self, n, me, own, slots, send, recv):
        self.n, self.me, self.own, self.slots = n, me, own, slots
        self.send, self.recv = send, recv
        self.core, self.chip = me % 2, me // 2
        self.partner = me + 1 - 2 * self.core
        self.started = []

    def copy(self, ident, src, dst, target):
        return pltpu.make_async_remote_copy(
            src_ref=src,
            dst_ref=dst,
            send_sem=self.send.at[ident],
            recv_sem=self.recv.at[ident],
            device_id={"ctx": target},
            device_id_type=MESH,
        )

    def peers(self):
        chips = self.n // 2
        if chips == 4:
            x, y = self.chip % 2, self.chip // 2
            nx, ny = y * 2 + (1 - x), (1 - y) * 2 + x
            return [(nx, nx), (ny, ny)]
        return [
            ((self.chip + d) % chips, (self.chip + chips - d) % chips) for d in range(1, chips)
        ]

    def begin(self):
        own_to = self.slots.at[self.me]
        self.first = [
            self.copy(i, self.own, own_to, to * 2 + self.core)
            for i, (to, _) in enumerate(self.peers())
        ]
        self.base = len(self.first)
        self.twin = self.copy(self.base, self.own, own_to, self.partner)
        for c in self.first:
            c.start()
        self.twin.start()
        self.started = self.first + [self.twin]

    def relay(self):
        here, self.passed, self.late = [], [], []
        ident = self.base + 1
        peers = self.peers()
        square = self.n // 2 == 4
        half = self.own.shape[0] // 2
        for i, (_, source) in enumerate(peers):
            self.first[i].wait_recv()
            block = source * 2 + self.core
            here.append(block)
            if square:
                piece = self.slots.at[block, pl.ds(i * half, half)]
                c = self.copy(ident, piece, piece, peers[1 - i][0] * 2 + self.core)
                c.start()
                self.late.append(c)
                ident += 1
            c = self.copy(ident, self.slots.at[block], self.slots.at[block], self.partner)
            c.start()
            self.passed.append((source * 2 + 1 - self.core, c))
            ident += 1
        self.ident = ident
        self.started += self.late + [c for _, c in self.passed]
        return here

    def diagonal(self):
        if not self.late:
            return None
        block = (3 - self.chip) * 2 + self.core
        half = self.own.shape[0] // 2
        self.last = []
        for i, c in enumerate(self.late):
            c.wait_recv()
            piece = self.slots.at[block, pl.ds(i * half, half)]
            c = self.copy(self.ident + i, piece, piece, self.partner)
            c.start()
            self.last.append(c)
        self.started += self.last
        return block

    def final(self):
        if not self.late:
            return None
        for c in self.last:
            c.wait_recv()
        return (3 - self.chip) * 2 + 1 - self.core

    def drain(self):
        for c in self.started:
            c.wait_send()


def gather_copies(n):
    return 9 if n // 2 == 4 else 2 * (n // 2) - 1


def attention_kernel(
    n,
    heads,
    x_ref,
    wq_ref,
    wk_ref,
    wv_ref,
    wo_ref,
    mixed_ref,
    wo_all,
    x_all,
    q_all,
    k_all,
    v_all,
    stage,
    x_send,
    x_recv,
    o_send,
    o_recv,
    m_send,
    m_recv,
):
    me = lax.axis_index("ctx")
    rows = x_ref.shape[0]
    barrier = pltpu.get_barrier_semaphore()
    for d in range(1, n):
        pl.semaphore_signal(
            barrier, inc=1, device_id={"ctx": (me + d) % n}, device_id_type=MESH
        )
    pl.semaphore_wait(barrier, n - 1)

    def project(block, value):
        at = pl.ds(pl.multiple_of(block * rows, rows), rows)
        for h in range(heads):
            cols = pl.ds(h * HS, HS)
            q_all[h, at, :] = jnp.dot(
                value, wq_ref[:, cols], preferred_element_type=jnp.float32
            ).astype(jnp.bfloat16)
            k_all[h, at, :] = jnp.dot(
                value, wk_ref[:, cols], preferred_element_type=jnp.float32
            ).astype(jnp.bfloat16)
        v_all[:, at] = lax.dot_general(
            wv_ref[...], value, (((1,), (1,)), ((), ())), preferred_element_type=jnp.float32
        ).astype(jnp.bfloat16)

    g = Gather(n, me, x_ref, x_all, x_send, x_recv)
    o = Gather(n, me, wo_ref, wo_all, o_send, o_recv)
    g.begin()
    project(me, x_ref[...])
    wo_all[me] = wo_ref[...]
    g.twin.wait_recv()
    project(g.partner, x_all[g.partner])
    here = g.relay()
    o.begin()
    for block in here:
        project(block, x_all[block])
    for block, c in g.passed:
        c.wait_recv()
        project(block, x_all[block])
    block = g.diagonal()
    if block is not None:
        project(block, x_all[block])
    o.twin.wait_recv()
    o.relay()
    block = g.final()
    if block is not None:
        project(block, x_all[block])

    scale = score_gain / math.sqrt(HS) * math.log2(math.e)

    def send_block(step, target):
        return pltpu.make_async_remote_copy(
            src_ref=stage.at[step],
            dst_ref=mixed_ref.at[me],
            send_sem=m_send.at[step],
            recv_sem=m_recv.at[step],
            device_id={"ctx": target},
            device_id_type=MESH,
        )

    @pl.loop(0, n)
    def _(step):
        block = lax.rem(me + 1 + step, n)
        at = pl.ds(pl.multiple_of(block * rows, rows), rows)
        for h in range(heads):
            scores = lax.dot_general(
                k_all[h],
                q_all[h, at, :],
                (((1,), (1,)), ((), ())),
                preferred_element_type=jnp.float32,
            )
            top = jnp.max(scores, axis=0, keepdims=True)
            weights = jnp.exp2(scores * scale - top * scale)
            total = jnp.sum(weights, axis=0, keepdims=True)
            cols = pl.ds(h * HS, HS)
            mixed = jnp.dot(
                v_all[cols, :],
                weights.astype(jnp.bfloat16),
                preferred_element_type=jnp.float32,
            )
            stage[step, cols, :] = (mixed / total).astype(jnp.bfloat16)

        @pl.when(step < n - 1)
        def _():
            send_block(step, block).start()

    mixed_ref[me] = stage[n - 1]
    for _, c in o.passed:
        c.wait_recv()
    o.diagonal()
    o.final()

    @pl.loop(0, n - 1)
    def _(step):
        send_block(step, lax.rem(me + 1 + step, n)).wait()

    g.drain()
    o.drain()


def attention(normed, w_query, w_key, w_value, w_out):
    n = lax.axis_size("ctx")
    rows, width = normed.shape
    inner = w_query.shape[1]
    heads = inner // HS
    copies = gather_copies(n)
    vmem = pl.BlockSpec(memory_space=pltpu.VMEM)
    bf = jnp.bfloat16
    return pl.pallas_call(
        functools.partial(attention_kernel, n, heads),
        out_shape=(
            jax.ShapeDtypeStruct((n, inner, rows), bf),
            jax.ShapeDtypeStruct((n,) + w_out.shape, bf),
        ),
        in_specs=[vmem] * 5,
        out_specs=(vmem, vmem),
        scratch_shapes=[
            pltpu.VMEM((n, rows, width), bf),
            pltpu.VMEM((heads, n * rows, HS), bf),
            pltpu.VMEM((heads, n * rows, HS), bf),
            pltpu.VMEM((inner, n * rows), bf),
            pltpu.VMEM((n, inner, rows), bf),
            pltpu.SemaphoreType.DMA((copies,)),
            pltpu.SemaphoreType.DMA((copies,)),
            pltpu.SemaphoreType.DMA((copies,)),
            pltpu.SemaphoreType.DMA((copies,)),
            pltpu.SemaphoreType.DMA((n,)),
            pltpu.SemaphoreType.DMA((n,)),
        ],
        compiler_params=pltpu.CompilerParams(collective_id=0, has_side_effects=True),
        name="attention",
    )(normed, w_query, w_key, w_value.T, w_out)


def experts(buffer, w_in, w_back, capacity):
    owners = lax.axis_size("dp") * lax.axis_size("ctx")
    expert_here, width = w_in.shape[0], buffer.shape[1]
    buffer = buffer.reshape(owners * expert_here, capacity, width)
    received = lax.all_to_all(buffer, ("dp", "ctx"), split_axis=0, concat_axis=0, tiled=True)
    grouped = received.reshape(owners, expert_here, capacity, width)
    hidden = jnp.einsum("sgid,gdf->sgif", grouped, w_in, preferred_element_type=jnp.float32)
    hidden = jnp.maximum(hidden, 0.0).astype(jnp.bfloat16)
    answer = jnp.einsum("sgif,gfd->sgid", hidden, w_back, preferred_element_type=jnp.float32)
    answered = answer.astype(jnp.bfloat16).reshape(owners * expert_here, capacity, width)
    back = lax.all_to_all(answered, ("dp", "ctx"), split_axis=0, concat_axis=0, tiled=True)
    return back.reshape(owners * expert_here * capacity, width)


def body(
    tokens, kept, gain_attn, gain_ffn, w_query, w_key, w_value, w_out, expert_ids, w_in, w_back
):
    document = tokens[0]
    shard_len, width_model = document.shape
    ctx_count = lax.axis_size("ctx")
    dp_count = lax.axis_size("dp")
    local = kept[0] - lax.axis_index("ctx") * shard_len
    keep_here = local.shape[0]
    rows = jnp.take(document, local, axis=0)
    normed = rms_scale(rows, gain_attn).astype(jnp.bfloat16)
    mixed, w_out_all = attention(normed, w_query, w_key, w_value, w_out)
    inner_all = w_out.shape[0] * ctx_count
    attn = lax.dot_general(
        mixed.reshape(inner_all, keep_here),
        w_out_all.reshape(inner_all, width_model),
        (((0,), (0,)), ((), ())),
        preferred_element_type=jnp.float32,
    )
    first = rows.astype(jnp.float32) + attn
    ffn_in = rms_scale(first, gain_ffn).astype(jnp.bfloat16)
    expert_here = w_in.shape[0]
    owners = dp_count * ctx_count
    experts_all = expert_here * owners
    capacity = 2 * keep_here // experts_all
    labels = expert_ids[0, :, 0]
    order = jnp.arange(keep_here, dtype=jnp.int32)
    same = (labels[:, None] == labels[None, :]) & (order[None, :] < order[:, None])
    slots = jnp.sum(same.astype(jnp.int32), axis=1)
    place = labels * capacity + slots
    cells = jnp.arange(experts_all * capacity, dtype=jnp.int32)
    spots = (place[None, :] == cells[:, None]).astype(jnp.bfloat16)
    buffer = jnp.dot(spots, ffn_in, preferred_element_type=jnp.float32).astype(jnp.bfloat16)
    answers = experts(buffer, w_in, w_back, capacity)
    seats = (place[:, None] == cells[None, :]).astype(jnp.bfloat16)
    taken = jnp.dot(seats, answers, preferred_element_type=jnp.float32)
    second = (first + taken).astype(jnp.bfloat16)
    hits = jnp.arange(shard_len, dtype=jnp.int32)[:, None] == local[None, :]
    fresh = jnp.dot(hits.astype(jnp.bfloat16), second, preferred_element_type=jnp.float32)
    touched = jnp.any(hits, axis=1, keepdims=True)
    blended = jnp.where(touched, fresh.astype(jnp.bfloat16), document)
    return blended[None]


def solution(mesh):
    return jax.shard_map(
        body,
        mesh=mesh,
        in_specs=(
            P("dp", "ctx", None),
            P("dp", "ctx"),
            P(),
            P(),
            P(None, "ctx"),
            P(None, "ctx"),
            P(None, "ctx"),
            P("ctx", None),
            P("dp", "ctx", None),
            P(("dp", "ctx"), None, None),
            P(("dp", "ctx"), None, None),
        ),
        out_specs=P("dp", "ctx", None),
        check_vma=False,
    )
```

```python
import functools
import math

import jax
import jax.numpy as jnp
from jax import lax
from jax.experimental import pallas as pl
from jax.experimental.pallas import tpu as pltpu
from jax.sharding import PartitionSpec as P

HS = 64
MESH = pl.DeviceIdType.MESH
LAST = (((1,), (1,)), ((), ()))

eps_norm = 1e-06
score_gain = 2.5


def rms_scale(values, gain):
    values = values.astype(jnp.float32)
    power = jnp.mean(values * values, axis=-1, keepdims=True)
    return values * lax.rsqrt(power + eps_norm) * gain


class Gather:
    def __init__(self, n, me, own, slots, send, recv):
        self.n, self.me, self.own, self.slots = n, me, own, slots
        self.send, self.recv = send, recv
        self.core, self.chip = me % 2, me // 2
        self.partner = me + 1 - 2 * self.core
        self.started = []

    def copy(self, ident, src, dst, target):
        return pltpu.make_async_remote_copy(
            src_ref=src,
            dst_ref=dst,
            send_sem=self.send.at[ident],
            recv_sem=self.recv.at[ident],
            device_id={"ctx": target},
            device_id_type=MESH,
        )

    def peers(self):
        chips = self.n // 2
        if chips == 4:
            x, y = self.chip % 2, self.chip // 2
            nx, ny = y * 2 + (1 - x), (1 - y) * 2 + x
            return [(nx, nx), (ny, ny)]
        return [
            ((self.chip + d) % chips, (self.chip + chips - d) % chips) for d in range(1, chips)
        ]

    def begin(self):
        own_to = self.slots.at[self.me]
        self.first = [
            self.copy(i, self.own, own_to, to * 2 + self.core)
            for i, (to, _) in enumerate(self.peers())
        ]
        self.base = len(self.first)
        self.twin = self.copy(self.base, self.own, own_to, self.partner)
        for c in self.first:
            c.start()
        self.twin.start()
        self.started = self.first + [self.twin]

    def relay(self):
        here, self.passed, self.late = [], [], []
        ident = self.base + 1
        peers = self.peers()
        square = self.n // 2 == 4
        half = self.own.shape[0] // 2
        for i, (_, source) in enumerate(peers):
            self.first[i].wait_recv()
            block = source * 2 + self.core
            here.append(block)
            if square:
                piece = self.slots.at[block, pl.ds(i * half, half)]
                c = self.copy(ident, piece, piece, peers[1 - i][0] * 2 + self.core)
                c.start()
                self.late.append(c)
                ident += 1
            c = self.copy(ident, self.slots.at[block], self.slots.at[block], self.partner)
            c.start()
            self.passed.append((source * 2 + 1 - self.core, c))
            ident += 1
        self.ident = ident
        self.started += self.late + [c for _, c in self.passed]
        return here

    def diagonal(self):
        if not self.late:
            return None
        block = (3 - self.chip) * 2 + self.core
        half = self.own.shape[0] // 2
        self.last = []
        for i, c in enumerate(self.late):
            c.wait_recv()
            piece = self.slots.at[block, pl.ds(i * half, half)]
            c = self.copy(self.ident + i, piece, piece, self.partner)
            c.start()
            self.last.append(c)
        self.started += self.last
        return block

    def final(self):
        if not self.late:
            return None
        for c in self.last:
            c.wait_recv()
        return (3 - self.chip) * 2 + 1 - self.core

    def drain(self):
        for c in self.started:
            c.wait_send()


def gather_copies(n):
    return 9 if n // 2 == 4 else 2 * (n // 2) - 1


def attention_kernel(
    n,
    heads,
    x_ref,
    wq_ref,
    wk_ref,
    wv_ref,
    wo_ref,
    mixed_ref,
    wo_all,
    x_all,
    q_all,
    k_all,
    v_all,
    stage,
    x_send,
    x_recv,
    o_send,
    o_recv,
    m_send,
    m_recv,
):
    me = lax.axis_index("ctx")
    rows = x_ref.shape[0]
    barrier = pltpu.get_barrier_semaphore()
    for d in range(1, n):
        pl.semaphore_signal(
            barrier, inc=1, device_id={"ctx": (me + d) % n}, device_id_type=MESH
        )
    pl.semaphore_wait(barrier, n - 1)

    def project(block, value):
        at = pl.ds(pl.multiple_of(block * rows, rows), rows)
        for h in range(heads):
            cols = pl.ds(h * HS, HS)
            q_all[h, at, :] = lax.dot_general(
                value, wq_ref[cols, :], LAST, preferred_element_type=jnp.float32
            ).astype(jnp.bfloat16)
            k_all[h, at, :] = lax.dot_general(
                value, wk_ref[cols, :], LAST, preferred_element_type=jnp.float32
            ).astype(jnp.bfloat16)
        v_all[:, at] = lax.dot_general(
            wv_ref[...], value, LAST, preferred_element_type=jnp.float32
        ).astype(jnp.bfloat16)

    g = Gather(n, me, x_ref, x_all, x_send, x_recv)
    o = Gather(n, me, wo_ref, wo_all, o_send, o_recv)
    g.begin()
    project(me, x_ref[...])
    wo_all[me] = wo_ref[...]
    g.twin.wait_recv()
    project(g.partner, x_all[g.partner])
    here = g.relay()
    o.begin()
    for block in here:
        project(block, x_all[block])
    for block, c in g.passed:
        c.wait_recv()
        project(block, x_all[block])
    block = g.diagonal()
    if block is not None:
        project(block, x_all[block])
    o.twin.wait_recv()
    o.relay()
    block = g.final()
    if block is not None:
        project(block, x_all[block])

    scale = score_gain / math.sqrt(HS) * math.log2(math.e)

    def send_block(step, target):
        return pltpu.make_async_remote_copy(
            src_ref=stage.at[step],
            dst_ref=mixed_ref.at[me],
            send_sem=m_send.at[step],
            recv_sem=m_recv.at[step],
            device_id={"ctx": target},
            device_id_type=MESH,
        )

    @pl.loop(0, n)
    def _(step):
        block = lax.rem(me + 1 + step, n)
        at = pl.ds(pl.multiple_of(block * rows, rows), rows)
        for h in range(heads):
            scores = lax.dot_general(
                k_all[h],
                q_all[h, at, :],
                LAST,
                preferred_element_type=jnp.float32,
            )
            top = jnp.max(scores, axis=0, keepdims=True)
            weights = jnp.exp2(scores * scale - top * scale)
            total = jnp.sum(weights, axis=0, keepdims=True)
            cols = pl.ds(h * HS, HS)
            mixed = jnp.dot(
                v_all[cols, :],
                weights.astype(jnp.bfloat16),
                preferred_element_type=jnp.float32,
            )
            stage[step, cols, :] = (mixed / total).astype(jnp.bfloat16)

        @pl.when(step < n - 1)
        def _():
            send_block(step, block).start()

    mixed_ref[me] = stage[n - 1]
    for _, c in o.passed:
        c.wait_recv()
    o.diagonal()
    o.final()

    @pl.loop(0, n - 1)
    def _(step):
        send_block(step, lax.rem(me + 1 + step, n)).wait()

    g.drain()
    o.drain()


def attention(normed, w_query, w_key, w_value, w_out):
    n = lax.axis_size("ctx")
    rows, width = normed.shape
    inner = w_query.shape[1]
    heads = inner // HS
    copies = gather_copies(n)
    vmem = pl.BlockSpec(memory_space=pltpu.VMEM)
    bf = jnp.bfloat16
    return pl.pallas_call(
        functools.partial(attention_kernel, n, heads),
        out_shape=(
            jax.ShapeDtypeStruct((n, inner, rows), bf),
            jax.ShapeDtypeStruct((n,) + w_out.shape, bf),
        ),
        in_specs=[vmem] * 5,
        out_specs=(vmem, vmem),
        scratch_shapes=[
            pltpu.VMEM((n, rows, width), bf),
            pltpu.VMEM((heads, n * rows, HS), bf),
            pltpu.VMEM((heads, n * rows, HS), bf),
            pltpu.VMEM((inner, n * rows), bf),
            pltpu.VMEM((n, inner, rows), bf),
            pltpu.SemaphoreType.DMA((copies,)),
            pltpu.SemaphoreType.DMA((copies,)),
            pltpu.SemaphoreType.DMA((copies,)),
            pltpu.SemaphoreType.DMA((copies,)),
            pltpu.SemaphoreType.DMA((n,)),
            pltpu.SemaphoreType.DMA((n,)),
        ],
        compiler_params=pltpu.CompilerParams(collective_id=0, has_side_effects=True),
        name="attention",
    )(normed, w_query.T, w_key.T, w_value.T, w_out)


def experts_plain(buffer, w_in, w_back, capacity):
    owners = lax.axis_size("dp") * lax.axis_size("ctx")
    expert_here, width = w_in.shape[0], buffer.shape[1]
    buffer = buffer.reshape(owners * expert_here, capacity, width)
    received = lax.all_to_all(buffer, ("dp", "ctx"), split_axis=0, concat_axis=0, tiled=True)
    grouped = received.reshape(owners, expert_here, capacity, width)
    hidden = jnp.einsum("sgid,gdf->sgif", grouped, w_in, preferred_element_type=jnp.float32)
    hidden = jnp.maximum(hidden, 0.0).astype(jnp.bfloat16)
    answer = jnp.einsum("sgif,gfd->sgid", hidden, w_back, preferred_element_type=jnp.float32)
    answered = answer.astype(jnp.bfloat16).reshape(owners * expert_here, capacity, width)
    back = lax.all_to_all(answered, ("dp", "ctx"), split_axis=0, concat_axis=0, tiled=True)
    return back.reshape(owners * expert_here * capacity, width)


def expert_kernel(
    planes,
    n,
    cap,
    buf_ref,
    w_in_hbm,
    w_back_hbm,
    back_ref,
    w_in_ref,
    w_back_ref,
    rows_ref,
    hidden_ref,
    answer_ref,
    w_sem,
    own_sem,
    d_send,
    d_recv,
    r_send,
    r_recv,
):
    dp, ctx = lax.axis_index("dp"), lax.axis_index("ctx")
    me = dp * n + ctx
    owners = planes * n
    loads = [
        pltpu.make_async_copy(w_in_hbm.at[0], w_in_ref, w_sem.at[0]),
        pltpu.make_async_copy(w_back_hbm.at[0], w_back_ref, w_sem.at[1]),
    ]
    for c in loads:
        c.start()
    barrier = pltpu.get_barrier_semaphore()

    @pl.loop(1, owners)
    def _(d):
        to = lax.rem(me + d, owners)
        pl.semaphore_signal(
            barrier, inc=1, device_id={"dp": to // n, "ctx": lax.rem(to, n)}, device_id_type=MESH
        )

    pl.semaphore_wait(barrier, owners - 1)

    def seat(index):
        return pl.ds(pl.multiple_of(index * cap, cap), cap)

    def at(shift):
        plane_shift, place_shift = shift // n, lax.rem(shift, n)
        half = planes // 2
        side = dp // half
        side = lax.rem(side + plane_shift // half, 2)
        plane = side * half + lax.rem(dp + plane_shift, half)
        return plane, lax.rem(ctx + place_shift, n)

    def dispatch(shift):
        plane, place = at(shift)
        return pltpu.make_async_remote_copy(
            src_ref=buf_ref.at[seat(plane * n + place)],
            dst_ref=rows_ref.at[seat(me)],
            send_sem=d_send.at[shift],
            recv_sem=d_recv.at[shift],
            device_id={"dp": plane, "ctx": place},
            device_id_type=MESH,
        )

    def give_back(shift):
        plane, place = at(shift)
        return pltpu.make_async_remote_copy(
            src_ref=answer_ref.at[seat(plane * n + place)],
            dst_ref=back_ref.at[seat(me)],
            send_sem=r_send.at[shift],
            recv_sem=r_recv.at[shift],
            device_id={"dp": plane, "ctx": place},
            device_id_type=MESH,
        )

    near = owners // 2

    @pl.loop(0, near)
    def _(shift):
        dispatch(near + shift).start()

        @pl.when(shift > 0)
        def _():
            dispatch(shift).start()

    own_in = pltpu.make_async_copy(buf_ref.at[seat(me)], rows_ref.at[seat(me)], own_sem.at[0])
    own_in.start()

    def run(first_row, count):
        inner = hidden_ref.shape[1]
        width = answer_ref.shape[1]
        take = pl.ds(pl.multiple_of(first_row, count), count)
        value = rows_ref[take, :]

        @pl.loop(0, inner // 256)
        def _(f):
            cols = pl.ds(pl.multiple_of(f * 256, 256), 256)
            hidden = jnp.dot(value, w_in_ref[:, cols], preferred_element_type=jnp.float32)
            hidden_ref[:, cols] = jnp.maximum(hidden, 0.0).astype(jnp.bfloat16)

        @pl.loop(0, width // 256)
        def _(f):
            cols = pl.ds(pl.multiple_of(f * 256, 256), 256)
            answer_ref[take, cols] = jnp.dot(
                hidden_ref[...], w_back_ref[:, cols], preferred_element_type=jnp.float32
            ).astype(jnp.bfloat16)

    half_rows = near * cap
    side = dp // (planes // 2)

    @pl.loop(1, near)
    def _(shift):
        dispatch(shift).wait_recv()

    own_in.wait()
    for c in loads:
        c.wait()

    @pl.loop(0, 2)
    def _(turn):
        @pl.when(turn == 1)
        def _():
            @pl.loop(near, owners)
            def _(shift):
                dispatch(shift).wait_recv()

        run(lax.rem(side + turn, 2) * half_rows, half_rows)

        @pl.loop(0, near)
        def _(shift):
            @pl.when(turn * near + shift > 0)
            def _():
                give_back(turn * near + shift).start()

    own_out = pltpu.make_async_copy(answer_ref.at[seat(me)], back_ref.at[seat(me)], own_sem.at[1])
    own_out.start()

    @pl.loop(1, owners)
    def _(shift):
        dispatch(shift).wait_send()
        give_back(shift).wait()

    own_out.wait()


def experts_fused(buffer, w_in, w_back, capacity):
    planes, n = lax.axis_size("dp"), lax.axis_size("ctx")
    owners = planes * n
    slots, width = buffer.shape
    inner = w_in.shape[2]
    bf = jnp.bfloat16
    vmem = pl.BlockSpec(memory_space=pltpu.VMEM)
    hbm = pl.BlockSpec(memory_space=pl.ANY)
    return pl.pallas_call(
        functools.partial(expert_kernel, planes, n, capacity),
        out_shape=jax.ShapeDtypeStruct((slots, width), bf),
        in_specs=[vmem, hbm, hbm],
        out_specs=vmem,
        scratch_shapes=[
            pltpu.VMEM(w_in.shape[1:], bf),
            pltpu.VMEM(w_back.shape[1:], bf),
            pltpu.VMEM((slots, width), bf),
            pltpu.VMEM((slots // 2, inner), bf),
            pltpu.VMEM((slots, width), bf),
            pltpu.SemaphoreType.DMA((2,)),
            pltpu.SemaphoreType.DMA((2,)),
            pltpu.SemaphoreType.DMA((owners,)),
            pltpu.SemaphoreType.DMA((owners,)),
            pltpu.SemaphoreType.DMA((owners,)),
            pltpu.SemaphoreType.DMA((owners,)),
        ],
        compiler_params=pltpu.CompilerParams(collective_id=1, has_side_effects=True),
        name="experts",
    )(buffer, w_in, w_back)


def experts(buffer, w_in, w_back, capacity):
    if capacity % 16 == 0 and w_in.shape[0] == 1:
        return experts_fused(buffer, w_in, w_back, capacity)
    return experts_plain(buffer, w_in, w_back, capacity)


def body(
    tokens, kept, gain_attn, gain_ffn, w_query, w_key, w_value, w_out, expert_ids, w_in, w_back
):
    document = tokens[0]
    shard_len, width_model = document.shape
    ctx_count = lax.axis_size("ctx")
    dp_count = lax.axis_size("dp")
    local = kept[0] - lax.axis_index("ctx") * shard_len
    keep_here = local.shape[0]
    positions = jnp.arange(shard_len, dtype=jnp.int32)
    picks = (local[:, None] == positions[None, :]).astype(jnp.bfloat16)
    rows = jnp.dot(picks, document, preferred_element_type=jnp.float32).astype(jnp.bfloat16)
    normed = rms_scale(rows, gain_attn).astype(jnp.bfloat16)
    mixed, w_out_all = attention(normed, w_query, w_key, w_value, w_out)
    inner_all = w_out.shape[0] * ctx_count
    attn = lax.dot_general(
        mixed.reshape(inner_all, keep_here),
        w_out_all.reshape(inner_all, width_model),
        (((0,), (0,)), ((), ())),
        preferred_element_type=jnp.float32,
    )
    first = rows.astype(jnp.float32) + attn
    ffn_in = rms_scale(first, gain_ffn).astype(jnp.bfloat16)
    expert_here = w_in.shape[0]
    owners = dp_count * ctx_count
    experts_all = expert_here * owners
    capacity = 2 * keep_here // experts_all
    labels = expert_ids[0, :, 0]
    order = jnp.arange(keep_here, dtype=jnp.int32)
    same = (labels[:, None] == labels[None, :]) & (order[None, :] < order[:, None])
    slots = jnp.sum(same.astype(jnp.int32), axis=1)
    place = labels * capacity + slots
    cells = jnp.arange(experts_all * capacity, dtype=jnp.int32)
    spots = (place[None, :] == cells[:, None]).astype(jnp.bfloat16)
    buffer = jnp.dot(spots, ffn_in, preferred_element_type=jnp.float32).astype(jnp.bfloat16)
    answers = experts(buffer, w_in, w_back, capacity)
    seats = (place[:, None] == cells[None, :]).astype(jnp.bfloat16)
    taken = jnp.dot(seats, answers, preferred_element_type=jnp.float32)
    second = (first + taken).astype(jnp.bfloat16)
    hits = positions[:, None] == local[None, :]
    fresh = jnp.dot(hits.astype(jnp.bfloat16), second, preferred_element_type=jnp.float32)
    touched = jnp.any(hits, axis=1, keepdims=True)
    blended = jnp.where(touched, fresh.astype(jnp.bfloat16), document)
    return blended[None]


def solution(mesh):
    return jax.shard_map(
        body,
        mesh=mesh,
        in_specs=(
            P("dp", "ctx", None),
            P("dp", "ctx"),
            P(),
            P(),
            P(None, "ctx"),
            P(None, "ctx"),
            P(None, "ctx"),
            P("ctx", None),
            P("dp", "ctx", None),
            P(("dp", "ctx"), None, None),
            P(("dp", "ctx"), None, None),
        ),
        out_specs=P("dp", "ctx", None),
        check_vma=False,
    )
```
